128 devices in a mesh: dp: 32 (over x, z, core), expert: 4 (over y).
Axes of the slice: x: 4, y: 4, z: 4, core: 2. Of those that a mesh axis runs over, the one named last changes fastest.
Arguments:
- tokens: bfloat16 [8192, 2048], P('dp'), may hold values from -6 to 6
- routes: int32 [8192, 6], P('dp'), may hold values from 0 to 63, all different within a row; in each aligned block of 256 rows (0 to 255, 256 to 511, ...) at most 32 rows name the same one
- gates: float32 [8192, 6], P('dp'), may hold values from 0.1 to 1
- w_gate: bfloat16 [64, 2048, 1408], P('dp', None, 'expert'), may hold values from -0.125 to 0.125
- w_up: bfloat16 [64, 2048, 1408], P('dp', None, 'expert'), may hold values from -0.125 to 0.125
- w_down: bfloat16 [64, 1408, 2048], P('dp', 'expert'), may hold values from -0.21875 to 0.21875
- s_gate: bfloat16 [2048, 2816], P(None, 'expert'), may hold values from -0.125 to 0.125
- s_up: bfloat16 [2048, 2816], P(None, 'expert'), may hold values from -0.125 to 0.125
- s_down: bfloat16 [2816, 2048], P('expert'), may hold values from -0.15625 to 0.15625
Outputs:
- mixed: bfloat16 [8192, 2048], P('dp', 'expert')
The draws below stay inside these ranges and needn't reach their ends.
Inputs may be any that keep to these rules, and one draw needn't show every extreme that they name: `routes`: each row names 6 different experts. Within each aligned block of 256 rows (the rows of one index of dp) no expert is named by more than 32 rows; some expert is named by exactly 32 rows in some block of every draw.
All inputs are finite; a program needn't handle non-finite values.
Results may differ from the reference program's by a relative error of at most 0.013.
Values may be sent and summed in bfloat16 or wider, within the bound.
No kernel may reach another device: no remote copies, remote signals or barrier semaphores. Data moves between devices by JAX's collectives and lax.ppermute only.
A program may use at most 128 MiB of HBM per device.

```python
import math
import jax
import jax.numpy as jnp
import numpy as np
from jax import lax

D = 2048
FF = 1408
SFF = 2816
EXPERTS = 64
TOP = 6
TOK_DEV = 256
CAP = 32
TOKENS = 8192
N_DP = 32
N_EXPERT = 4


def strengthened(values, own_key, source, target, shards_of, factor):
    def block_of(axis_at):
        return (jnp.arange(values.shape[axis_at]) // (values.shape[axis_at] // shards_of)).reshape((-1,) + (1,) * (values.ndim - 1 - axis_at))

    near = jax.random.permutation(own_key, shards_of)[block_of(target)]
    second = (block_of(target) + shards_of // 2) % shards_of
    return jnp.where((block_of(source) == near) | (block_of(source) == second), factor * values, values)


def level_of(rng, extent, shards, least, largest):
    def one(axis_at, blocks):
        steps = jax.random.uniform(jax.random.fold_in(jax.random.fold_in(rng, 6), axis_at), (blocks,), jnp.float32, least / len(shards), largest / len(shards))
        return jnp.repeat(jnp.exp(steps), extent[axis_at] // blocks).reshape((-1,) + (1,) * (len(extent) - axis_at - 1))

    gain = one(*shards[0])
    for cut in shards[1:]:
        gain = gain * one(*cut)
    return gain


def assign_block(rng, own, number, rows, amount, top, reach, lean):
    ranking = jax.random.permutation(rng, amount)
    heavy_load, common = shares(amount, rows * top, reach, lean, True), shares(amount, rows * top, reach, lean, False)
    places = jnp.arange(amount)

    def named(sizes, turn):
        used = int((sizes > 0).sum())
        fixed = max(1, used // 4)
        moved = fixed + (places - fixed + turn * (used - fixed)) % max(1, amount - fixed)
        return jnp.zeros((amount,), jnp.int32).at[ranking[jnp.where(places < fixed, places, moved)]].set(jnp.asarray(sizes, jnp.int32))

    sizes = jnp.where(number % 4 == 0, named(heavy_load, number // 4), named(common, number - number // 4 - 1))
    mixed = jax.random.permutation(jax.random.fold_in(own, 3), amount)
    donor, taker = mixed[0:amount // 2 * 2:2], mixed[1:amount // 2 * 2:2]
    room = jnp.minimum(sizes[donor] - 1, reach - sizes[taker]) // 2
    room = jnp.where((donor == ranking[0]) | (taker == ranking[0]) | (sizes[taker] == 0), 0, jnp.maximum(room, 0))
    moved = jax.random.randint(jax.random.fold_in(own, 4), (amount // 2,), 0, 1 << 20) % (room + 1)
    sizes = sizes.at[donor].add(-moved).at[taker].add(moved)
    members = jnp.searchsorted(jnp.cumsum(sizes), jnp.arange(rows * top), side="right").astype(jnp.int32)
    grid = members.reshape(top, rows).T
    grid = grid[jax.random.permutation(jax.random.fold_in(own, 1), rows)]
    turn = jax.random.randint(jax.random.fold_in(own, 2), (rows, 1), 0, top)
    return jnp.take_along_axis(grid, (jnp.arange(top)[None, :] + turn) % top, axis=1)


def shares(amount, total, most, skew, full):
    weights = [(1 << 20) // math.isqrt(standing ** skew) + 1 for standing in range(1, amount + 1)]
    largest = most if full else min(most, max(-(-total // amount), total * weights[0] // sum(weights)))
    least = 1 if total - largest >= amount - 1 else 0
    given, spare = [largest] + [least] * (amount - 1), total - largest - least * (amount - 1)
    while spare > 0:
        candidates = [i for i in range(1, amount) if given[i] < largest] or [i for i in range(1, amount) if given[i] < most]
        mass, left = sum([weights[i] for i in candidates]), spare
        for i in candidates:
            more = min(most - given[i], max(1, left * weights[i] // mass), spare)
            given[i] = given[i] + more
            spare = spare - more
    return np.array(given)


def noise(rng, extent, deviation, reach, split=(), kind=jnp.bfloat16):
    gain = level_of(rng, extent, split, -0.22, 0.18) if split else 1.0
    array = jax.random.normal(rng, extent, jnp.float32) * deviation * gain
    return jnp.minimum(jnp.maximum(array, -reach), reach).astype(kind)


def bell_draw_with(own_key, dims, spread, bound, split, heavy, kind=jnp.bfloat16):
    result = spread * jax.random.normal(own_key, dims, jnp.float32)
    if split:
        result = result * level_of(own_key, dims, split, -0.22, 0.18)
    return jnp.clip(strengthened(result, jax.random.fold_in(own_key, 3), *heavy), -bound, bound).astype(kind)


def setup_inputs(seed: int = 0) -> dict:
    splits = jax.random.split(jax.random.key(seed), 10)
    tokens = noise(splits[0], (TOKENS, D), 1.0, 6.0, ((0, 32),))
    routes_keys = jax.random.split(jax.random.fold_in(splits[1], 1), TOKENS // TOK_DEV)
    routes_turns = jax.random.permutation(jax.random.fold_in(splits[1], 3), TOKENS // TOK_DEV)
    routes = jax.vmap(lambda own, number: assign_block(jax.random.fold_in(splits[1], 2), own, number, TOK_DEV, EXPERTS, TOP, CAP, 2))(routes_keys, routes_turns).reshape((TOKENS, TOP))
    gates = jnp.clip(jnp.exp(math.log(1.0) - 2.3025851 * jax.random.uniform(splits[2], (TOKENS, TOP), jnp.float32) ** level_of(splits[2], (TOKENS, TOP), ((0, 32),), -0.2, 0.2)), 0.1, 1.0)
    w_gate = noise(splits[3], (EXPERTS, D, FF), D ** -0.5, 0.125, ((0, 32), (2, 4)))
    w_up = noise(splits[4], (EXPERTS, D, FF), D ** -0.5, 0.125, ((0, 32), (2, 4)))
    w_down = bell_draw_with(splits[5], (EXPERTS, FF, D), FF ** -0.5, 0.21875, ((0, 32), (1, 4)), (1, 2, 4, 2.0))
    s_gate = noise(splits[6], (D, SFF), D ** -0.5, 0.125, ((1, 4),))
    s_up = noise(splits[7], (D, SFF), D ** -0.5, 0.125, ((1, 4),))
    s_down = bell_draw_with(splits[8], (SFF, D), SFF ** -0.5, 0.15625, ((0, 4),), (0, 1, 4, 2.0))
    return {"tokens": tokens, "routes": routes, "gates": gates, "w_gate": w_gate, "w_up": w_up, "w_down": w_down, "s_gate": s_gate, "s_up": s_up, "s_down": s_down}


def quarter_sum(hidden, down, parts):
    inner = hidden.shape[1] // parts
    partial_value = jnp.einsum("rqf,qfd->rqd", hidden.reshape(hidden.shape[0], parts, inner).astype(jnp.float32), down.reshape(parts, inner, down.shape[1]).astype(jnp.float32))
    rounded = lax.optimization_barrier(partial_value.astype(jnp.bfloat16))
    return jnp.sum(rounded.astype(jnp.float32), axis=1)


def reference(tokens, routes, gates, w_gate, w_up, w_down, s_gate, s_up, s_down):
    blocks = routes.reshape(N_DP, TOK_DEV, TOP)
    labels = jnp.arange(EXPERTS, dtype=jnp.int32)
    matches = (blocks[:, :, :, None] == labels[None, None, None, :]).astype(jnp.int32)
    counts = jnp.sum(matches, axis=2).astype(jnp.int32)
    before = (jnp.cumsum(counts, axis=1) - counts).astype(jnp.int32)
    slots = jnp.sum(matches * before[:, :, None, :], axis=3).astype(jnp.int32)
    owner_block = jnp.arange(N_DP, dtype=jnp.int32)[:, None, None]
    dest = ((blocks * N_DP + owner_block) * CAP + slots).astype(jnp.int32)
    token_ids = owner_block * TOK_DEV + jnp.arange(TOK_DEV, dtype=jnp.int32)[None, :, None] + jnp.zeros((1, 1, TOP), jnp.int32)
    sources = jnp.full((EXPERTS * N_DP * CAP,), TOKENS, jnp.int32).at[dest.reshape(-1)].set(token_ids.reshape(-1).astype(jnp.int32))
    padded = jnp.concatenate([tokens, jnp.zeros((1, D), tokens.dtype)], axis=0)

    def one_expert(inputs):
        table, gate_w, up_w, down_w = inputs
        rows = padded[table]
        gate = jnp.dot(rows, gate_w, preferred_element_type=jnp.float32)
        up = jnp.dot(rows, up_w, preferred_element_type=jnp.float32)
        hidden = (jax.nn.silu(gate) * up).astype(jnp.bfloat16)
        return quarter_sum(hidden, down_w, N_EXPERT).astype(jnp.bfloat16)

    outputs = lax.map(one_expert, (sources.reshape(EXPERTS, N_DP * CAP), w_gate, w_up, w_down))
    flat = outputs.reshape(EXPERTS * N_DP * CAP, D)
    picked = flat[dest.reshape(TOKENS, TOP)].astype(jnp.float32)
    routed = jnp.einsum("tk,tkd->td", gates.astype(jnp.float32), picked)
    shared_gate = jnp.dot(tokens, s_gate, preferred_element_type=jnp.float32)
    shared_up = jnp.dot(tokens, s_up, preferred_element_type=jnp.float32)
    shared_hidden = (jax.nn.silu(shared_gate) * shared_up).astype(jnp.bfloat16)
    shared_out = quarter_sum(shared_hidden, s_down, N_EXPERT)
    return (shared_out + routed).astype(jnp.bfloat16)
```

```python
import functools
import jax
import jax.numpy as jnp
from jax import lax
from jax.experimental import pallas as pl
from jax.experimental.pallas import tpu as pltpu
from jax.sharding import Mesh, PartitionSpec as P

CAP = 32
BF = jnp.bfloat16
F32 = jnp.float32
ORDER = (1, 3, 2)
MIB = 1024 * 1024


def shift(value, axis, by):
    return lax.ppermute(value, axis, [(i, (i + by) % 4) for i in range(4)])


def swap_core(value):
    return lax.ppermute(value, "c", [(0, 1), (1, 0)])


def pair_a(value):
    return lax.ppermute(value, "y", [(i, i ^ 1) for i in range(4)])


def pair_b(value):
    return lax.ppermute(value, "y", [(i, 3 - i) for i in range(4)])


def call(kernel, outs, *operands, limit=32, scalars=None, scratch=()):
    vm = pl.BlockSpec(memory_space=pltpu.VMEM)
    specs = [vm] * len(operands)
    if scalars is not None:
        operands = (scalars,) + operands
        specs = [pl.BlockSpec(memory_space=pltpu.SMEM)] + specs
    return pl.pallas_call(
        kernel,
        out_shape=[jax.ShapeDtypeStruct(s, d) for s, d in outs],
        in_specs=specs,
        out_specs=[vm] * len(outs),
        scratch_shapes=list(scratch),
        compiler_params=pltpu.CompilerParams(vmem_limit_bytes=limit * MIB),
    )(*operands)


def nt(a, b):
    return lax.dot_general(a, b, (((1,), (1,)), ((), ())), preferred_element_type=F32)


def nn(a, b):
    return lax.dot_general(a, b, (((1,), (0,)), ((), ())), preferred_element_type=F32)


def tn(a, b):
    return lax.dot_general(a, b, (((0,), (0,)), ((), ())), preferred_element_type=F32)


def pack_kernel(where, routes, gates, tokens, *outs):
    x, z, c, a, b = (where[i] for i in range(5))
    rows = lax.broadcasted_iota(jnp.int32, (64, 256), 0)
    far, cc, near, j = rows >> 4, (rows >> 3) & 1, (rows >> 1) & 3, rows & 1
    t_from = lax.broadcasted_iota(jnp.int32, (256, 256), 0)
    t_to = lax.broadcasted_iota(jnp.int32, (256, 256), 1)
    earlier = (t_from < t_to).astype(F32).astype(BF)
    for which in range(2):
        if which == 0:
            dest = ((x + far) & 3) * 8 + ((z + near) & 3) * 2
            column = a
        else:
            dest = ((x + near) & 3) * 8 + ((z + far) & 3) * 2
            column = b
        ids = (dest + (c ^ cc)) * 2 + j
        named = jnp.zeros((64, 256), F32)
        weight = jnp.zeros((64, 256), F32)
        for k in range(6):
            hit = routes[k : k + 1, :] == ids
            named = jnp.where(hit, 1.0, named)
            weight = jnp.where(hit, gates[k : k + 1, :], weight)
        before = nn(named.astype(BF), earlier)
        code = jnp.where(named > 0.5, before, -1.0)
        own = tokens[:, pl.ds(pl.multiple_of(column * 512, 512), 512)]
        for d in range(4):
            out = outs[which * 4 + d]
            out[0:256, :] = own
            for half in range(2):
                at = d * 16 + half * 8
                table = jnp.concatenate([code[at : at + 8], weight[at : at + 8]], axis=0)
                out[256:272, half * 256 : half * 256 + 256] = table.astype(BF)


def tables(payload, half):
    table = payload[256:272, half * 256 : half * 256 + 256].astype(F32)
    spread = lambda v: jnp.broadcast_to(v[:, None, :], (8, CAP, 256)).reshape(8 * CAP, 256)
    return spread(table[0:8]), spread(table[8:16])


def slot_rows():
    return (lax.broadcasted_iota(jnp.int32, (8 * CAP, 256), 0) % CAP).astype(F32)


def select_kernel(*refs):
    payloads, outs = refs[:8], refs[8:]
    slots = slot_rows()
    for cs in range(2):
        for d in range(4):
            payload = payloads[cs * 4 + d]
            code, _ = tables(payload, cs)
            chosen = (code == slots).astype(F32).astype(BF)
            rows = nn(chosen, payload[0:256, :]).astype(BF)
            at = (d * 2 + cs) * CAP
            for near in range(4):
                for j in range(2):
                    r = (near * 2 + j) * CAP
                    outs[j * 4 + near][at : at + CAP, :] = rows[r : r + CAP]


def expert_kernel(where, *refs):
    own_a, own_b, got_a, got_b = refs[0:4], refs[4:8], refs[8:12], refs[12:16]
    w_gate, w_up, w_down = refs[16:19]
    keep_a, keep_b, give_a, give_b = refs[19:23]
    at = [pl.multiple_of(where[i] * 512, 512) for i in range(4)]
    for dz in range(4):
        by_x = lambda blocks: jnp.concatenate([blocks[dx][dz * 64 : dz * 64 + 64, :] for dx in range(4)], axis=0)
        pieces = (own_a[dz][...], by_x(own_b), got_a[dz][...], by_x(got_b))
        gate = up = None
        for piece, start in zip(pieces, at):
            g = nt(piece, w_gate[0, :, pl.ds(start, 512)])
            u = nt(piece, w_up[0, :, pl.ds(start, 512)])
            gate = g if gate is None else gate + g
            up = u if up is None else up + u
        hidden = (gate / (1.0 + jnp.exp(-gate)) * up).astype(BF)
        for start, out, on_x in zip(at, (keep_a, keep_b, give_a, give_b), (False, True, False, True)):
            value = nn(hidden, w_down[0, :, pl.ds(start, 512)]).astype(BF)
            if on_x:
                for dx in range(4):
                    out[dx * 256 + dz * 64 : dx * 256 + dz * 64 + 64, :] = value[dx * 64 : dx * 64 + 64]
            else:
                out[dz * 256 : dz * 256 + 256, :] = value


def shared_kernel(where, tokens, s_gate, s_up, s_down, *outs):
    gate = nt(tokens[...], s_gate[...])
    up = nt(tokens[...], s_up[...])
    hidden = (gate / (1.0 + jnp.exp(-gate)) * up).astype(BF)
    for i in range(4):
        start = pl.multiple_of(where[i] * 512, 512)
        outs[i][...] = nn(hidden, s_down[:, pl.ds(start, 512)]).astype(BF)


def add_kernel(left, right, *outs):
    rows = left.shape[0] // len(outs)
    for i, out in enumerate(outs):
        at = slice(i * rows, i * rows + rows)
        out[...] = (left[at, :].astype(F32) + right[at, :].astype(F32)).astype(BF)


def combine_kernel(*refs):
    payloads, values, outs = refs[:8], refs[8:16], refs[16:]
    slots = slot_rows()
    for cs in range(2):
        for d in range(4):
            code, weight = tables(payloads[cs * 4 + d], cs)
            mixing = jnp.where(code == slots, weight, 0.0).astype(BF)
            at = (d * 2 + cs) * CAP
            rows = jnp.concatenate(
                [values[j * 4 + near][at : at + CAP, :] for near in range(4) for j in range(2)], axis=0
            )
            outs[cs * 4 + d][...] = tn(mixing, rows).astype(BF)


def total_kernel(*refs):
    out = refs[-1]
    acc = refs[0][...].astype(F32)
    for ref in refs[1:-1]:
        acc = acc + ref[...].astype(F32)
    out[...] = acc.astype(out.dtype)


def body(tokens, routes, gates, w_gate, w_up, w_down, s_gate, s_up, s_down):
    x, z, c, y = (lax.axis_index(n).astype(jnp.int32) for n in ("x", "z", "c", "y"))
    a = 3 * (y & 1)
    b = 1 + (y >> 1)
    here = jnp.stack([x, z, c, a, b])
    blocks = jnp.stack([a, b, 3 - a, 3 - b])

    sent = call(pack_kernel, [((272, 512), BF)] * 8, routes.T, gates.T, tokens, scalars=here)
    own, other = {}, {}
    for s, axis in enumerate("xz"):
        own[s, 0] = sent[s * 4]
    for d in ORDER:
        for s, axis in enumerate("xz"):
            own[s, d] = shift(sent[s * 4 + d], axis, d)
    for d in (0,) + ORDER:
        for s in range(2):
            other[s, d] = swap_core(own[s, d])

    sets = []
    for s in range(2):
        sets.append([own[s, d] for d in range(4)] + [other[s, d] for d in range(4)])
    chosen = [call(select_kernel, [((256, 512), BF)] * 8, *sets[s]) for s in range(2)]

    shared = call(
        shared_kernel, [((256, 512), BF)] * 4, tokens, s_gate.T, s_up.T, s_down, scalars=blocks
    )
    shared_got = (pair_a(shared[2]), pair_b(shared[3]))

    pairs = (pair_a, pair_b)
    gate_t, up_t = jnp.swapaxes(w_gate, 1, 2), jnp.swapaxes(w_up, 1, 2)
    back = {}
    for j in range(2):
        mine, got = {}, {}
        for d in (0,) + ORDER:
            for s, axis in enumerate("zx"):
                value = chosen[s][j * 4 + d]
                mine[s, d] = value if d == 0 else shift(value, axis, d)
                got[s, d] = pairs[s](mine[s, d])
        order = [mine[s, d] for s in range(2) for d in range(4)] + [got[s, d] for s in range(2) for d in range(4)]
        result = call(
            expert_kernel,
            [((1024, 512), BF)] * 4,
            *order,
            gate_t[j : j + 1],
            up_t[j : j + 1],
            w_down[j : j + 1],
            scalars=blocks,
            limit=40,
        )
        for s, axis in enumerate("zx"):
            summed = call(add_kernel, [((256, 512), BF)] * 4, result[s], pairs[s](result[2 + s]))
            for d in range(4):
                back[s, j, d] = summed[d] if d == 0 else shift(summed[d], axis, -d)

    finals = []
    for s, axis in enumerate("xz"):
        mixed = call(
            combine_kernel,
            [((256, 512), BF)] * 8,
            *sets[s],
            *[back[s, j, d] for j in range(2) for d in range(4)],
        )
        parts = []
        for d in range(4):
            (whole,) = call(add_kernel, [((256, 512), BF)], mixed[d], swap_core(mixed[4 + d]))
            parts.append(whole if d == 0 else shift(whole, axis, -d))
        (final,) = call(total_kernel, [((256, 512), BF)], *parts, shared[s], shared_got[s])
        finals.append(final)

    on_a = (y == 0) | (y == 3)
    keep = jnp.where(on_a, finals[0], finals[1])
    give = jnp.where(on_a, finals[1], finals[0])
    received = lax.ppermute(give, "y", [(0, 1), (1, 3), (2, 0), (3, 2)])
    return (keep.astype(F32) + received.astype(F32)).astype(BF)


def solution(mesh):
    grid = Mesh(mesh.devices.reshape(4, 4, 2, 4), ("x", "z", "c", "y"))
    dp = ("x", "z", "c")
    placed = (
        P(dp, None),
        P(dp, None),
        P(dp, None),
        P(dp, None, "y"),
        P(dp, None, "y"),
        P(dp, "y", None),
        P(None, "y"),
        P(None, "y"),
        P("y", None),
    )
    return jax.shard_map(body, mesh=grid, in_specs=placed, out_specs=P(dp, "y"), check_vma=False)
```

```python
import functools
import jax
import jax.numpy as jnp
from jax import lax
from jax.experimental import pallas as pl
from jax.experimental.pallas import tpu as pltpu
from jax.sharding import Mesh, PartitionSpec as P


CAP = 32
BF = jnp.bfloat16
F32 = jnp.float32
ORDER = (1, 3, 2)
MIB = 1024 * 1024


def shift(value, axis, by):
    return lax.ppermute(value, axis, [(i, (i + by) % 4) for i in range(4)])


def swap_core(value):
    return lax.ppermute(value, "c", [(0, 1), (1, 0)])


def pair_a(value):
    return lax.ppermute(value, "y", [(i, i ^ 1) for i in range(4)])


def pair_b(value):
    return lax.ppermute(value, "y", [(i, 3 - i) for i in range(4)])


def call(kernel, outs, *operands, limit=16, scalars=None, flops=1e8, raw=False, scratch=()):
    vm = pl.BlockSpec(memory_space=pltpu.VMEM)
    specs = [pl.BlockSpec(memory_space=pltpu.HBM) if raw else vm] * len(operands)
    if scalars is not None:
        operands = (scalars,) + operands
        specs = [pl.BlockSpec(memory_space=pltpu.SMEM)] + specs
    return pl.pallas_call(
        kernel,
        out_shape=[o if isinstance(o, jax.ShapeDtypeStruct) else jax.ShapeDtypeStruct(o, BF) for o in outs],
        in_specs=specs,
        out_specs=[vm] * len(outs),
        scratch_shapes=list(scratch),
        compiler_params=pltpu.CompilerParams(vmem_limit_bytes=limit * MIB),
        cost_estimate=pl.CostEstimate(flops=int(flops), bytes_accessed=1 << 20, transcendentals=0),
    )(*operands)


def nt(a, b):
    return lax.dot_general(a, b, (((1,), (1,)), ((), ())), preferred_element_type=F32)


def nn(a, b):
    return lax.dot_general(a, b, (((1,), (0,)), ((), ())), preferred_element_type=F32)


def tn(a, b):
    return lax.dot_general(a, b, (((0,), (0,)), ((), ())), preferred_element_type=F32)


def pack_kernel(where, routes_in, gates_in, tokens, *refs):
    outs, (routes, gates, columns, sems) = refs[:8], refs[8:]
    x, z, c, a, b = (where[i] for i in range(5))
    copies = [pltpu.make_async_copy(routes_in, routes, sems.at[0]), pltpu.make_async_copy(gates_in, gates, sems.at[1])]
    for which, column in enumerate((a, b)):
        part = tokens.at[:, pl.ds(pl.multiple_of(column * 512, 512), 512)]
        copies.append(pltpu.make_async_copy(part, columns.at[which], sems.at[2 + which]))
    for copy in copies:
        copy.start()
    copies[0].wait()
    copies[1].wait()
    rows = lax.broadcasted_iota(jnp.int32, (64, 256), 0)
    far, cc, near, j = rows >> 4, (rows >> 3) & 1, (rows >> 1) & 3, rows & 1
    t_from = lax.broadcasted_iota(jnp.int32, (256, 256), 0)
    t_to = lax.broadcasted_iota(jnp.int32, (256, 256), 1)
    earlier = (t_from < t_to).astype(F32).astype(BF)
    for which in range(2):
        if which == 0:
            dest = ((x + far) & 3) * 8 + ((z + near) & 3) * 2
        else:
            dest = ((x + near) & 3) * 8 + ((z + far) & 3) * 2
        ids = (dest + (c ^ cc)) * 2 + j
        named = jnp.zeros((64, 256), F32)
        weight = jnp.zeros((64, 256), F32)
        for k in range(6):
            hit = routes[k : k + 1, :] == ids
            named = jnp.where(hit, 1.0, named)
            weight = jnp.where(hit, gates[k : k + 1, :], weight)
        before = nn(named.astype(BF), earlier)
        code = jnp.where(named > 0.5, before, -1.0)
        copies[2 + which].wait()
        for d in range(4):
            out = outs[which * 4 + d]
            out[0:256, :] = columns[which]
            for half in range(2):
                at = d * 16 + half * 8
                table = jnp.concatenate([code[at : at + 8], weight[at : at + 8]], axis=0)
                out[256:272, half * 256 : half * 256 + 256] = table.astype(BF)


def tables(payload, half):
    table = payload[256:272, half * 256 : half * 256 + 256].astype(F32)
    spread = lambda v: jnp.broadcast_to(v[:, None, :], (8, CAP, 256)).reshape(8 * CAP, 256)
    return spread(table[0:8]), spread(table[8:16])


def slot_rows():
    return (lax.broadcasted_iota(jnp.int32, (8 * CAP, 256), 0) % CAP).astype(F32)


def select_kernel(*refs):
    payloads, outs = refs[:8], refs[8:]
    slots = slot_rows()
    for cs in range(2):
        for d in range(4):
            payload = payloads[cs * 4 + d]
            code, _ = tables(payload, cs)
            chosen = (code == slots).astype(F32).astype(BF)
            rows = nn(chosen, payload[0:256, :]).astype(BF)
            at = (d * 2 + cs) * CAP
            for near in range(4):
                for j in range(2):
                    r = (near * 2 + j) * CAP
                    outs[near][j * 256 + at : j * 256 + at + CAP, :] = rows[r : r + CAP]


def product(piece, weights, j, at):
    return nt(piece, weights[j, :, pl.ds(pl.multiple_of(at * 512, 512), 512)])


def own_kernel(where, *refs):
    own_a, own_b, (w_gate, w_up, gate, up) = refs[0:4], refs[4:8], refs[8:]

    @pl.loop(0, 2)
    def _(j):
        base = pl.multiple_of(j * 256, 256)
        for dz in range(4):
            piece_a = own_a[dz][pl.ds(base, 256), :]
            piece_b = jnp.concatenate([own_b[dx][pl.ds(base + dz * 64, 64), :] for dx in range(4)], axis=0)
            for weights, out in ((w_gate, gate), (w_up, up)):
                out[j, dz] = product(piece_a, weights, j, where[0]) + product(piece_b, weights, j, where[1])


def accumulate(where, got_a, got_b, d, j, weights, acc):
    base = pl.multiple_of(j * 256, 256)
    acc[j, d] += product(got_a[pl.ds(base, 256), :], weights, j, where[2])
    by_x = product(got_b[pl.ds(base, 256), :], weights, j, where[3])
    for dz in range(4):
        acc[j, dz, d * 64 : d * 64 + 64, :] += by_x[dz * 64 : dz * 64 + 64]


def more_kernel(where, *refs):
    got, (w_gate, w_up, gate_in, up_in, gate, up) = refs[0:6], refs[6:]
    gate[...] = gate_in[...]
    up[...] = up_in[...]

    @pl.loop(0, 2)
    def _(j):
        for i, d in enumerate((0, 1, 3)):
            for weights, out in ((w_gate, gate), (w_up, up)):
                accumulate(where, got[i], got[3 + i], d, j, weights, out)


def hidden_kernel(where, got_a, got_b, w_gate, w_up, gate_in, up_in, hidden, gate, up):
    gate[...] = gate_in[...]
    up[...] = up_in[...]

    @pl.loop(0, 2)
    def _(j):
        accumulate(where, got_a, got_b, 2, j, w_gate, gate)
        accumulate(where, got_a, got_b, 2, j, w_up, up)
        g = gate[j]
        hidden[j] = (g / (1.0 + jnp.exp(-g)) * up[j]).astype(BF)


def down(where, hidden, w_down, j, i, d):
    if i % 2 == 0:
        rows = hidden[j, d]
    else:
        rows = jnp.concatenate([hidden[j, dz, d * 64 : d * 64 + 64, :] for dz in range(4)], axis=0)
    start = pl.multiple_of(where[i] * 512, 512)
    return nn(rows, w_down[j, :, pl.ds(start, 512)]).astype(BF)


def down_kernel(picks, where, hidden, w_down, *outs):
    @pl.loop(0, 2)
    def _(j):
        for (i, d), out in zip(picks, outs):
            out[pl.ds(pl.multiple_of(j * 256, 256), 256), :] = down(where, hidden, w_down, j, i, d)


def shared_kernel(where, tokens, s_gate, s_up, s_down, *outs):
    gate = nt(tokens[...], s_gate[...])
    up = nt(tokens[...], s_up[...])
    hidden = (gate / (1.0 + jnp.exp(-gate)) * up).astype(BF)
    for i in range(4):
        start = pl.multiple_of(where[i] * 512, 512)
        outs[i][...] = nn(hidden, s_down[:, pl.ds(start, 512)]).astype(BF)


def add_kernel(left, right, *outs):
    rows = left.shape[0] // len(outs)
    for i, out in enumerate(outs):
        at = slice(i * rows, i * rows + rows)
        out[...] = (left[at, :].astype(F32) + right[at, :].astype(F32)).astype(BF)


def combine_kernel(*refs):
    payloads, values, outs = refs[:8], refs[8:12], refs[12:]
    slots = slot_rows()
    for cs in range(2):
        for d in range(4):
            code, weight = tables(payloads[cs * 4 + d], cs)
            mixing = jnp.where(code == slots, weight, 0.0).astype(BF)
            at = (d * 2 + cs) * CAP
            rows = jnp.concatenate(
                [values[near][j * 256 + at : j * 256 + at + CAP, :] for near in range(4) for j in range(2)], axis=0
            )
            value = tn(mixing, rows).astype(BF)
            if cs == 0:
                outs[0][d * 256 : d * 256 + 256, :] = value
            else:
                outs[1][d * 256 : d * 256 + 256, :] = value


def total_kernel(where, *refs):
    keep, give = refs[-2:]
    sums = []
    for s in range(2):
        parts = refs[s * 6 : s * 6 + 6]
        acc = parts[0][...].astype(F32)
        for ref in parts[1:]:
            acc = acc + ref[...].astype(F32)
        sums.append(acc)
    on_a = (where[0] == 0) == (where[1] == 1)
    keep[...] = jnp.where(on_a, sums[0], sums[1])
    give[...] = jnp.where(on_a, sums[1], sums[0]).astype(BF)


def last_kernel(left, right, out):
    out[...] = (left[...] + right[...].astype(F32)).astype(BF)


def body(tokens, routes, gates, w_gate, w_up, w_down, s_gate, s_up, s_down):
    x, z, c, y = (lax.axis_index(n).astype(jnp.int32) for n in ("x", "z", "c", "y"))
    a = 3 * (y & 1)
    b = 1 + (y >> 1)
    here = jnp.stack([x, z, c, a, b])
    blocks = jnp.stack([a, b, 3 - a, 3 - b])

    sent = call(
        pack_kernel,
        [(272, 512)] * 8,
        routes.T,
        gates.T,
        tokens,
        scalars=here,
        raw=True,
        scratch=(
            pltpu.VMEM((6, 256), jnp.int32),
            pltpu.VMEM((6, 256), F32),
            pltpu.VMEM((2, 256, 512), BF),
            pltpu.SemaphoreType.DMA((4,)),
        ),
    )
    own, other = {}, {}
    for s in range(2):
        own[s, 0] = sent[s * 4]
    for d in ORDER:
        for s, axis in enumerate("xz"):
            own[s, d] = shift(sent[s * 4 + d], axis, d)
    for d in (0,) + ORDER:
        for s in range(2):
            other[s, d] = swap_core(own[s, d])

    shared = call(shared_kernel, [(256, 512)] * 4, tokens, s_gate.T, s_up.T, s_down, scalars=blocks, flops=2e9)
    pairs = (pair_a, pair_b)
    shared_got = []
    for s in range(2):
        shared_got.append(pairs[s](shared[2 + s]))

    sets, mine, got = [], {}, {}
    for s, axis in enumerate("zx"):
        sets.append([own[s, d] for d in range(4)] + [other[s, d] for d in range(4)])
        chosen = call(select_kernel, [(512, 512)] * 4, *sets[s], flops=6e8)
        for d in (0, 1, 3, 2):
            mine[s, d] = chosen[d] if d == 0 else shift(chosen[d], axis, d)
            got[s, d] = pairs[s](mine[s, d])
    every = [(s, d) for s in range(2) for d in range(4)]
    weights = jnp.swapaxes(w_gate, 1, 2), jnp.swapaxes(w_up, 1, 2)
    shape = (2, 4, 256, w_gate.shape[2])
    wide = jax.ShapeDtypeStruct(shape, F32)
    sums = call(own_kernel, [wide] * 2, *[mine[k] for k in every], *weights, scalars=blocks, flops=6e9)
    early = [got[s, d] for s in range(2) for d in (0, 1, 3)]
    sums = call(more_kernel, [wide] * 2, *early, *weights, *sums, scalars=blocks, flops=6e9)
    (hidden,) = call(
        hidden_kernel,
        [shape],
        got[0, 2],
        got[1, 2],
        *weights,
        *sums,
        scalars=blocks,
        flops=2e9,
        scratch=(pltpu.VMEM(shape, F32), pltpu.VMEM(shape, F32)),
    )
    first = [(2, 2), (3, 2)]
    rest = [(i, d) for d in (1, 3, 0) for i in (2, 3)] + [(i, d) for d in (2, 1, 3, 0) for i in (0, 1)]
    result = {}
    for picks in (first, rest):
        kernel = functools.partial(down_kernel, picks)
        values = call(kernel, [(512, 512)] * len(picks), hidden, w_down, scalars=blocks, flops=3e9)
        result.update(zip(picks, values))
    back = {}
    for d in (2, 1, 3, 0):
        for s, axis in enumerate("zx"):
            came = pairs[s](result[2 + s, d])
            (summed,) = call(add_kernel, [(512, 512)], result[s, d], came)
            back[s, d] = summed if d == 0 else shift(summed, axis, -d)

    finals = []
    for s, axis in enumerate("xz"):
        mixed = call(combine_kernel, [(1024, 512)] * 2, *sets[s], *[back[s, d] for d in range(4)], flops=6e8)
        came = swap_core(mixed[1])
        whole = call(add_kernel, [(256, 512)] * 4, mixed[0], came)
        parts = [whole[0]]
        for d in ORDER:
            parts.append(shift(whole[d], axis, -d))
        finals += [*parts, shared[s], shared_got[s]]

    block = (256, 512)
    keep, give = call(total_kernel, [jax.ShapeDtypeStruct(block, F32), block], *finals, scalars=blocks)
    received = lax.ppermute(give, "y", [(0, 1), (1, 3), (2, 0), (3, 2)])
    (out,) = call(last_kernel, [block], keep, received)
    return out


def solution(mesh):
    grid = Mesh(mesh.devices.reshape(4, 4, 2, 4), ("x", "z", "c", "y"))
    dp = ("x", "z", "c")
    placed = (
        P(dp, None),
        P(dp, None),
        P(dp, None),
        P(dp, None, "y"),
        P(dp, None, "y"),
        P(dp, "y", None),
        P(None, "y"),
        P(None, "y"),
        P("y", None),
    )
    return jax.shard_map(body, mesh=grid, in_specs=placed, out_specs=P(dp, "y"), check_vma=False)
```

```python
import functools
import jax
import jax.numpy as jnp
from jax import lax
from jax.experimental import pallas as pl
from jax.experimental.pallas import tpu as pltpu
from jax.sharding import Mesh, PartitionSpec as P


CAP = 32
BF = jnp.bfloat16
F32 = jnp.float32
ORDER = (1, 3, 2)
DIRECT = (1, 2, 3)
MIB = 1024 * 1024


def shift(value, axis, by):
    return lax.ppermute(value, axis, [(i, (i + by) % 4) for i in range(4)])


def swap_core(value):
    return lax.ppermute(value, "c", [(0, 1), (1, 0)])


def pair_a(value):
    return lax.ppermute(value, "y", [(i, i ^ 1) for i in range(4)])


def pair_b(value):
    return lax.ppermute(value, "y", [(i, 3 - i) for i in range(4)])


def call(kernel, outs, *operands, limit=16, scalars=None, flops=1e8, raw=False, scratch=(), aliases=None):
    vm = pl.BlockSpec(memory_space=pltpu.VMEM)
    specs = [pl.BlockSpec(memory_space=pltpu.HBM) if raw else vm] * len(operands)
    if scalars is not None:
        operands = (scalars,) + operands
        specs = [pl.BlockSpec(memory_space=pltpu.SMEM)] + specs
    return pl.pallas_call(
        kernel,
        out_shape=[o if isinstance(o, jax.ShapeDtypeStruct) else jax.ShapeDtypeStruct(o, BF) for o in outs],
        in_specs=specs,
        out_specs=[vm] * len(outs),
        scratch_shapes=list(scratch),
        input_output_aliases=aliases or {},
        compiler_params=pltpu.CompilerParams(vmem_limit_bytes=limit * MIB),
        cost_estimate=pl.CostEstimate(flops=int(flops), bytes_accessed=1 << 20, transcendentals=0),
    )(*operands)


def nt(a, b):
    return lax.dot_general(a, b, (((1,), (1,)), ((), ())), preferred_element_type=F32)


def nn(a, b):
    return lax.dot_general(a, b, (((1,), (0,)), ((), ())), preferred_element_type=F32)


def tn(a, b):
    return lax.dot_general(a, b, (((0,), (0,)), ((), ())), preferred_element_type=F32)


def pack_kernel(where, routes_in, gates_in, tokens, *refs):
    outs, (routes, gates, columns, sems) = refs[:8], refs[8:]
    x, z, c, a, b = (where[i] for i in range(5))
    copies = [pltpu.make_async_copy(routes_in, routes, sems.at[0]), pltpu.make_async_copy(gates_in, gates, sems.at[1])]
    for which, column in enumerate((a, b, 3 - a, 3 - b)):
        part = tokens.at[:, pl.ds(pl.multiple_of(column * 512, 512), 512)]
        copies.append(pltpu.make_async_copy(part, columns.at[which], sems.at[2 + which]))
    for copy in copies:
        copy.start()
    copies[0].wait()
    copies[1].wait()
    rows = lax.broadcasted_iota(jnp.int32, (64, 256), 0)
    far, cc, near, j = rows >> 4, (rows >> 3) & 1, (rows >> 1) & 3, rows & 1
    t_from = lax.broadcasted_iota(jnp.int32, (256, 256), 0)
    t_to = lax.broadcasted_iota(jnp.int32, (256, 256), 1)
    earlier = (t_from < t_to).astype(F32).astype(BF)
    for which in range(2):
        if which == 0:
            dest = ((x + far) & 3) * 8 + ((z + near) & 3) * 2
        else:
            dest = ((x + near) & 3) * 8 + ((z + far) & 3) * 2
        ids = (dest + (c ^ cc)) * 2 + j
        named = jnp.zeros((64, 256), F32)
        weight = jnp.zeros((64, 256), F32)
        for k in range(6):
            hit = routes[k : k + 1, :] == ids
            named = jnp.where(hit, 1.0, named)
            weight = jnp.where(hit, gates[k : k + 1, :], weight)
        before = nn(named.astype(BF), earlier)
        code = jnp.where(named > 0.5, before, -1.0)
        copies[2 + which].wait()
        copies[4 + which].wait()
        outs[which * 4][272:528, :] = columns[2 + which]
        for d in range(4):
            out = outs[which * 4 + d]
            out[0:256, :] = columns[which]
            for half in range(2):
                at = d * 16 + half * 8
                table = jnp.concatenate([code[at : at + 8], weight[at : at + 8]], axis=0)
                out[256:272, half * 256 : half * 256 + 256] = table.astype(BF)


def tables(payload, half):
    table = payload[256:272, half * 256 : half * 256 + 256].astype(F32)
    spread = lambda v: jnp.broadcast_to(v[:, None, :], (8, CAP, 256)).reshape(8 * CAP, 256)
    return spread(table[0:8]), spread(table[8:16])


def slot_rows():
    return (lax.broadcasted_iota(jnp.int32, (8 * CAP, 256), 0) % CAP).astype(F32)


def place(e, j):
    return 384 + j * 64 if e == 0 else j * 192 + (e - 1) * 64


def select_kernel(*refs):
    payloads, outs = refs[:8], refs[8:]
    slots = slot_rows()
    for cs in range(2):
        for e in range(4):
            payload = payloads[cs * 4 + e]
            code, _ = tables(payload, cs)
            chosen = (code == slots).astype(F32).astype(BF)
            rows = nn(chosen, payload[0:256, :]).astype(BF)
            both = nn(chosen, payload[272:528, :]).astype(BF) if e == 0 else None
            for near in range(4):
                for j in range(2):
                    r = (near * 2 + j) * CAP
                    at = place(e, j) + cs * CAP
                    outs[near][at : at + CAP, :] = rows[r : r + CAP]
                    if e == 0 and near in DIRECT:
                        outs[near][at + 128 : at + 128 + CAP, :] = both[r : r + CAP]


def whole_rows(block, j):
    return jnp.concatenate([block[pl.ds(384 + j * 64, 64), :], block[pl.ds(j * 192, 192), :]], axis=0)


def product(piece, weights, j, at):
    return nt(piece, weights[j, :, pl.ds(pl.multiple_of(at * 512, 512), 512)])


def add_own(where, own_a, own_b, picks, j, weights, acc):
    piece_a = jnp.concatenate([whole_rows(block, j) for block in own_a], axis=0)
    piece_b = jnp.concatenate([whole_rows(block, j) for block in own_b], axis=0)
    from_a = product(piece_a, weights, j, where[0])
    from_b = product(piece_b, weights, j, where[1])
    for i, d in enumerate(picks):
        if len(picks) > 1:
            acc[j, d] = from_a[i * 256 : i * 256 + 256]
        else:
            acc[j, d] += from_a
    for i, d in enumerate(picks):
        for dz in range(4):
            acc[j, dz, d * 64 : d * 64 + 64, :] += from_b[i * 256 + dz * 64 : i * 256 + dz * 64 + 64]
    direct = [(block_a, block_b, d) for block_a, block_b, d in zip(own_a, own_b, picks) if d in DIRECT]
    if not direct:
        return
    piece_a = jnp.concatenate([block[pl.ds(512 + j * 64, 64), :] for block, _, _ in direct], axis=0)
    piece_b = jnp.concatenate([block[pl.ds(512 + j * 64, 64), :] for _, block, _ in direct], axis=0)
    from_a = product(piece_a, weights, j, where[2])
    from_b = product(piece_b, weights, j, where[3])
    for i, (_, _, d) in enumerate(direct):
        acc[j, d, 0:64, :] += from_a[i * 64 : i * 64 + 64]
        acc[j, 0, d * 64 : d * 64 + 64, :] += from_b[i * 64 : i * 64 + 64]


def own_kernel(where, *refs):
    own, (w_gate, w_up, gate, up) = refs[0:6], refs[6:]

    @pl.loop(0, 2)
    def _(j):
        for weights, acc in ((w_gate, gate), (w_up, up)):
            acc[j, 2] = jnp.zeros(acc.shape[2:], F32)
            add_own(where, own[0:3], own[3:6], (0, 1, 3), j, weights, acc)


def came_rows(block, d, j):
    return block[pl.ds(j * 192, 192), :] if d in DIRECT else whole_rows(block, j)


def accumulate(where, got_a, got_b, d, j, weights, acc):
    skip = 64 if d in DIRECT else 0
    acc[j, d, skip:256, :] += product(came_rows(got_a, d, j), weights, j, where[2])
    extra = product(came_rows(got_b, d, j), weights, j, where[3])
    for dz in range(skip // 64, 4):
        acc[j, dz, d * 64 : d * 64 + 64, :] += extra[dz * 64 - skip : dz * 64 + 64 - skip]


def more_kernel(where, *refs):
    own, got, (w_gate, w_up, _, _, gate, up) = refs[0:2], refs[2:8], refs[8:]

    @pl.loop(0, 2)
    def _(j):
        for weights, out in ((w_gate, gate), (w_up, up)):
            add_own(where, own[0:1], own[1:2], (2,), j, weights, out)
            for i, d in enumerate((0, 1, 3)):
                accumulate(where, got[i], got[3 + i], d, j, weights, out)


def down(where, hidden, w_down, j, i, d, outs):
    if i % 2 == 0:
        rows = hidden[j, d]
    else:
        rows = jnp.concatenate([hidden[j, dz, d * 64 : d * 64 + 64, :] for dz in range(4)], axis=0)
    start = pl.multiple_of(where[i] * 512, 512)
    value = nn(rows, w_down[j, :, pl.ds(start, 512)]).astype(BF)
    outs[0][pl.ds(j * 192, 192), :] = value[64:256]
    if len(outs) == 1:
        outs[0][pl.ds(384 + j * 64, 64), :] = value[0:64]
    else:
        outs[1][pl.ds(j * 64, 64), :] = value[0:64]


def down_shapes(picks):
    shapes = []
    for i, d in picks:
        shapes += [(512, 512)] if i < 2 or d not in DIRECT else [(384, 512), (128, 512)]
    return shapes


def down_outs(picks, outs):
    taken, result = 0, {}
    for i, d in picks:
        count = 1 if i < 2 or d not in DIRECT else 2
        result[i, d] = outs[taken : taken + count]
        taken += count
    return result


def hidden_kernel(picks, where, got_a, got_b, w_gate, w_up, gate, up, w_down, hidden, *refs):
    outs = down_outs(picks, refs)

    @pl.loop(0, 2)
    def _(j):
        skip = 64 if 2 in DIRECT else 0
        from_a = [product(came_rows(got_a, 2, j), w, j, where[2]) for w in (w_gate, w_up)]
        from_b = [product(came_rows(got_b, 2, j), w, j, where[3]) for w in (w_gate, w_up)]
        for dz in range(4):
            for e in range(4):
                at = slice(e * 64, e * 64 + 64)
                sums = []
                for i, acc in enumerate((gate, up)):
                    value = acc[j, dz, at, :]
                    if dz == 2 and e * 64 >= skip:
                        value = value + from_a[i][e * 64 - skip : e * 64 + 64 - skip]
                    if e == 2 and dz * 64 >= skip:
                        value = value + from_b[i][dz * 64 - skip : dz * 64 + 64 - skip]
                    sums.append(value)
                g, u = sums
                hidden[j, dz, at, :] = (g / (1.0 + jnp.exp(-g)) * u).astype(BF)
        for i, d in picks:
            down(where, hidden, w_down, j, i, d, outs[i, d])


def down_kernel(picks, where, hidden, w_down, *refs):
    outs = down_outs(picks, refs)

    @pl.loop(0, 2)
    def _(j):
        for i, d in picks:
            down(where, hidden, w_down, j, i, d, outs[i, d])


def shared_kernel(where, tokens, s_gate, s_up, s_down, *outs):
    gate = nt(tokens[...], s_gate[...])
    up = nt(tokens[...], s_up[...])
    hidden = (gate / (1.0 + jnp.exp(-gate)) * up).astype(BF)
    for i in range(4):
        start = pl.multiple_of(where[i] * 512, 512)
        outs[i][...] = nn(hidden, s_down[:, pl.ds(start, 512)]).astype(BF)


def add_kernel(left, right, *refs):
    out = refs[-1]
    count = right.shape[0]
    out[0:count, :] = (left[0:count, :].astype(F32) + right[...].astype(F32)).astype(BF)
    if count < 512:
        out[count:512, :] = left[count:512, :]
        out[512:640, :] = refs[0][...]


def combine_kernel(*refs):
    payloads, values, (mine, other, direct) = refs[:8], refs[8:12], refs[12:]
    slots = slot_rows()
    for cs in range(2):
        for e in range(4):
            code, weight = tables(payloads[cs * 4 + e], cs)
            mixing = jnp.where(code == slots, weight, 0.0).astype(BF)
            at = [place(e, j) + cs * CAP for j in range(2)]
            rows = jnp.concatenate(
                [values[near][at[j] : at[j] + CAP, :] for near in range(4) for j in range(2)], axis=0
            )
            (mine, other)[cs][e * 256 : e * 256 + 256, :] = tn(mixing, rows).astype(BF)
            if e == 0:
                rows = jnp.concatenate(
                    [values[near][at[j] + 128 : at[j] + 128 + CAP, :] for near in DIRECT for j in range(2)],
                    axis=0,
                )
                weights = jnp.concatenate([mixing[near * 64 : near * 64 + 64] for near in DIRECT], axis=0)
                value = tn(weights, rows).astype(BF)
                if cs == 0:
                    direct[...] = value
                else:
                    other[1024:1280, :] = value


def both_kernel(left, direct, shared, right, *outs):
    for e in range(4):
        at = slice(e * 256, e * 256 + 256)
        outs[e][...] = (left[at, :].astype(F32) + right[at, :].astype(F32)).astype(BF)
    outs[4][...] = (direct[...].astype(F32) + shared[...].astype(F32) + right[1024:1280, :].astype(F32)).astype(BF)


def total_kernel(where, *refs):
    keep, give = refs[-2:]
    sums = []
    for s in range(2):
        parts = refs[s * 6 : s * 6 + 6]
        acc = parts[0][...].astype(F32)
        for ref in parts[1:]:
            acc = acc + ref[...].astype(F32)
        sums.append(acc)
    on_a = (where[0] == 0) == (where[1] == 1)
    keep[...] = jnp.where(on_a, sums[0], sums[1])
    give[...] = jnp.where(on_a, sums[1], sums[0]).astype(BF)


def last_kernel(left, right, out):
    out[...] = (left[...] + right[...].astype(F32)).astype(BF)


def body(tokens, routes, gates, w_gate, w_up, w_down, s_gate, s_up, s_down):
    x, z, c, y = (lax.axis_index(n).astype(jnp.int32) for n in ("x", "z", "c", "y"))
    a = 3 * (y & 1)
    b = 1 + (y >> 1)
    here = jnp.stack([x, z, c, a, b])
    blocks = jnp.stack([a, b, 3 - a, 3 - b])

    sent = call(
        pack_kernel,
        [(272 if i % 4 else 528, 512) for i in range(8)],
        routes.T,
        gates.T,
        tokens,
        scalars=here,
        raw=True,
        scratch=(
            pltpu.VMEM((6, 256), jnp.int32),
            pltpu.VMEM((6, 256), F32),
            pltpu.VMEM((4, 256, 512), BF),
            pltpu.SemaphoreType.DMA((6,)),
        ),
    )
    own, other = {}, {}
    for s in range(2):
        own[s, 0] = sent[s * 4]
    for d in ORDER:
        for s, axis in enumerate("xz"):
            own[s, d] = shift(sent[s * 4 + d], axis, d)
    for d in (0,) + ORDER:
        for s in range(2):
            other[s, d] = swap_core(own[s, d])

    shared = call(shared_kernel, [(256, 512)] * 4, tokens, s_gate.T, s_up.T, s_down, scalars=blocks, flops=2e9)
    pairs = (pair_a, pair_b)
    sets, mine, got = [], {}, {}
    for s, axis in enumerate("zx"):
        sets.append([own[s, d] for d in range(4)] + [other[s, d] for d in range(4)])
        chosen = call(select_kernel, [(640 if d in DIRECT else 512, 512) for d in range(4)], *sets[s], flops=6e8)
        for d in (0, 1, 3, 2):
            mine[s, d] = chosen[d] if d == 0 else shift(chosen[d], axis, d)
            got[s, d] = pairs[s](mine[s, d][:384] if d in DIRECT else mine[s, d])
    weights = jnp.swapaxes(w_gate, 1, 2), jnp.swapaxes(w_up, 1, 2)
    shape = (2, 4, 256, w_gate.shape[2])
    wide = jax.ShapeDtypeStruct(shape, F32)
    early = [(s, d) for s in range(2) for d in (0, 1, 3)]
    sums = call(own_kernel, [wide] * 2, *[mine[k] for k in early], *weights, scalars=blocks, flops=5e9)
    sums = call(
        more_kernel,
        [wide] * 2,
        mine[0, 2],
        mine[1, 2],
        *[got[k] for k in early],
        *weights,
        *sums,
        scalars=blocks,
        flops=6e9,
        aliases={11: 0, 12: 1},
    )
    first = [(2, 2), (3, 2)]
    rest = [(i, d) for d in (1, 3, 0) for i in (2, 3)] + [(i, d) for d in (2, 1, 3, 0) for i in (0, 1)]
    hidden, *given = call(
        functools.partial(hidden_kernel, first),
        [shape] + down_shapes(first),
        got[0, 2],
        got[1, 2],
        *weights,
        *sums,
        w_down,
        scalars=blocks,
        flops=3e9,
    )
    result = down_outs(first, given)
    kernel = functools.partial(down_kernel, rest)
    result |= down_outs(rest, call(kernel, down_shapes(rest), hidden, w_down, scalars=blocks, flops=3e9))
    back = {}
    for d in (2, 1, 3, 0):
        for s, axis in enumerate("zx"):
            away, *direct = result[2 + s, d]
            came = pairs[s](away)
            size = (640 if d in DIRECT else 512, 512)
            (summed,) = call(add_kernel, [size], result[s, d][0], came, *direct)
            back[s, d] = summed if d == 0 else shift(summed, axis, -d)

    finals = []
    for s, axis in enumerate("xz"):
        own_part, other_part, direct = call(
            combine_kernel, [(1024, 512), (1280, 512), (256, 512)], *sets[s], *[back[s, d] for d in range(4)], flops=6e8
        )
        came = swap_core(other_part)
        whole = call(both_kernel, [(256, 512)] * 5, own_part, direct, shared[2 + s], came)
        parts = [whole[0]]
        for d in ORDER:
            parts.append(shift(whole[d], axis, -d))
        parts.append(pairs[s](whole[4]))
        finals += [*parts, shared[s]]

    block = (256, 512)
    keep, give = call(total_kernel, [jax.ShapeDtypeStruct(block, F32), block], *finals, scalars=blocks)
    received = lax.ppermute(give, "y", [(0, 1), (1, 3), (2, 0), (3, 2)])
    (out,) = call(last_kernel, [block], keep, received)
    return out


def solution(mesh):
    grid = Mesh(mesh.devices.reshape(4, 4, 2, 4), ("x", "z", "c", "y"))
    dp = ("x", "z", "c")
    placed = (
        P(dp, None),
        P(dp, None),
        P(dp, None),
        P(dp, None, "y"),
        P(dp, None, "y"),
        P(dp, "y", None),
        P(None, "y"),
        P(None, "y"),
        P("y", None),
    )
    return jax.shard_map(body, mesh=grid, in_specs=placed, out_specs=P(dp, "y"), check_vma=False)
```
